32 devices in a mesh: rep: 2 (over z, core), dp: 16 (over x, y).
Axes of the slice: x: 4, y: 4, z: 1, core: 2. Of those that a mesh axis runs over, the one named last changes fastest.
The devices are a block of a 4x4x8 slice.
Arguments:
- a: bfloat16 [32, 4, 4096, 640], P(('rep', 'dp')), parts along dimension 0
- g: bfloat16 [32, 4, 4096, 2560], P(('rep', 'dp')), parts along dimension 0
Outputs:
- output: bfloat16 [8, 640, 2560], P('rep'), parts along dimension 0
There are 2 independent parts. The reference program is written for one: setup_inputs(seed, part) draws one part's arguments, and reference() takes and returns one part's arrays. A program takes and returns all parts, laid end to end along the dimension named above; each array names one.
All inputs are finite; a program needn't handle non-finite values.
Results may differ from the reference program's by a relative error of at most 0.012.
Values are sent between devices in bfloat16 or wider.
A program may use at most 768 MiB of HBM per device.

```python
import jax
import jax.numpy as jnp
from jax import lax

DEVICES = 16
MATRICES = 4
TOKENS = 4096
D = 640
FF = 2560


def setup_inputs(seed: int = 0, part: int = 0) -> dict:
    ka, kg, ks = (jax.random.fold_in(k, part) for k in jax.random.split(jax.random.key(seed), 3))
    size = 2.0 ** jax.random.uniform(ks, (DEVICES, MATRICES, 1, 1), jnp.float32, -1.0, 1.0)
    a = jax.random.normal(ka, (DEVICES, MATRICES, TOKENS, D), jnp.float32)
    g = size * jax.random.normal(kg, (DEVICES, MATRICES, TOKENS, FF), jnp.float32) * (DEVICES * TOKENS) ** -0.5
    return {"a": a.astype(jnp.bfloat16), "g": g.astype(jnp.bfloat16)}


def reference(a, g):
    def take(so_far, one):
        return so_far + jnp.einsum("ntd,ntf->ndf", *one, preferred_element_type=jnp.float32), None

    return lax.scan(take, jnp.zeros((MATRICES, D, FF), jnp.float32), (a, g))[0].astype(jnp.bfloat16)
```

```python
import jax
import jax.numpy as jnp
from jax import lax
from jax.sharding import PartitionSpec as P


def solution(mesh):
    def body(a, g):
        outs = []
        for n in range(a.shape[1]):
            term = lax.dot_general(a[0, n], g[0, n], (((0,), (0,)), ((), ())), preferred_element_type=jnp.float32)
            term = term.astype(jnp.bfloat16)
            if outs:
                term, outs[-1] = lax.optimization_barrier((term, outs[-1]))
            outs.append(lax.psum(term, "dp"))
        return jnp.stack(outs)

    spec = P(("rep", "dp"), None, None, None)
    return jax.shard_map(body, mesh=mesh, in_specs=(spec, spec), out_specs=P("rep", None, None), check_vma=False)
```

```python
import functools
import math

import jax
import jax.numpy as jnp
from jax import lax
from jax.experimental import pallas as pl
from jax.experimental.pallas import tpu as pltpu
from jax.sharding import PartitionSpec as P

LANES = 128
SLOTS = 4
PIECES = 4
G_SLOTS = 3
HOLD = 3


def kernel(side, a_hbm, g_hbm, out, a_buf, g_buf, acc, part, mine, *rest):
    send_bufs, recv_bufs = rest[:4], rest[4:8]
    a_sem, g_sem, send_sem, recv_sem = rest[8:]
    matrices, tokens, rows = a_hbm.shape[1:]
    width = side * LANES
    per_matrix = g_hbm.shape[3] // width
    chunks = matrices * per_matrix
    half1, rows2 = rows // 2, rows // side
    half2 = rows2 // 2
    me = lax.axis_index("dp")
    x, y = me // side, me % side
    bf16, f32 = jnp.bfloat16, jnp.float32

    class Chunk:
        def __init__(self, c):
            odd = c % 2
            self.c, self.slot = c, c % SLOTS
            self.matrix = c // per_matrix
            self.column = (c % per_matrix) * width
            self.p = x * (1 - odd) + y * odd
            self.q = y * (1 - odd) + x * odd
            self.stride1 = side * (1 - odd) + odd
            self.stride2 = side * odd + 1 - odd

        def first(self, d):
            return (self.p + d + side) % side * self.stride1 + self.q * self.stride2

        def second(self, d):
            return self.p * self.stride1 + (self.q + d + side) % side * self.stride2

        def term(self, d, half):
            s = (self.p + d + side) % side
            lanes = pl.ds(pl.multiple_of(s * LANES, LANES), LANES)
            return acc[self.c % 2, half * half1 : (half + 1) * half1, lanes]

        def sub(self, d, half):
            s = (self.q + d + side) % side
            return part[self.slot, pl.ds(pl.multiple_of(s * rows2 + half * half2, half2), half2), :]

        def block(self, d1, start, size):
            s = (self.p + d1 + side) % side
            lanes = pl.ds(pl.multiple_of(self.column + s * LANES, LANES), LANES)
            return out.at[self.matrix, pl.ds(pl.multiple_of(start, 16), size), lanes]

        def copy(self, stage, way):
            to = 1 - 2 * way
            if stage < 4:
                src, dst = send_bufs[stage].at[self.slot, way], recv_bufs[stage].at[self.slot, way]
                device = self.first(to) if stage < 2 else self.second(to)
            elif stage == 4:
                src = dst = self.block(0, self.q * rows2, rows2)
                device = self.second(to)
            elif stage == 5:
                src = dst = self.block(0, (self.q - to + side) % side * rows2 + way * half2, half2)
                device = self.second(to)
            elif stage == 6:
                src = dst = self.block(0, 0, rows)
                device = self.first(to)
            else:
                src = dst = self.block(-to, way * half1, half1)
                device = self.first(to)
            return pltpu.make_async_remote_copy(
                src_ref=src,
                dst_ref=dst,
                send_sem=send_sem.at[stage, way, self.slot],
                recv_sem=recv_sem.at[stage, way, self.slot],
                device_id={"dp": device},
                device_id_type=pl.DeviceIdType.MESH,
            )

        def send(self, stage):
            for way in range(2):
                self.copy(stage, way).start()

        def received(self, stage):
            for way in range(2):
                self.copy(stage, way).wait_recv()

        def sent(self, stage):
            for way in range(2):
                self.copy(stage, way).wait_send()

    def a_copies(n):
        depth = tokens // PIECES
        for i in range(PIECES):
            piece = pl.ds(i * depth, depth)
            yield pltpu.make_async_copy(a_hbm.at[0, n, piece, :], a_buf.at[n % 2, piece, :], a_sem.at[n % 2, i])

    def g_copies(c):
        depth = tokens // PIECES
        lanes = pl.ds(pl.multiple_of(c % per_matrix * width, width), width)
        for i in range(PIECES):
            piece = pl.ds(i * depth, depth)
            yield pltpu.make_async_copy(
                g_hbm.at[0, c // per_matrix, piece, lanes], g_buf.at[c % G_SLOTS, piece, :], g_sem.at[c % G_SLOTS, i]
            )

    def multiply(c):
        k = Chunk(c)

        @pl.when(c % per_matrix == 0)
        def _():
            for copy in a_copies(k.matrix):
                copy.wait()

            @pl.when(k.matrix + 1 < matrices)
            def _():
                for copy in a_copies(k.matrix + 1):
                    copy.start()

        for copy in g_copies(c):
            copy.wait()

        @pl.when(c + 2 < chunks)
        def _():
            for copy in g_copies(c + 2):
                copy.start()

        acc[c % 2] = lax.dot_general(
            a_buf[k.matrix % 2], g_buf[c % G_SLOTS], (((0,), (0,)), ((), ())), preferred_element_type=f32
        )
        buf = send_bufs[0]
        buf[k.slot, 0, :half1] = k.term(2, 0).astype(bf16)
        buf[k.slot, 0, half1:] = k.term(1, 1).astype(bf16)
        buf[k.slot, 1, :half1] = k.term(-1, 0).astype(bf16)
        buf[k.slot, 1, half1:] = k.term(2, 1).astype(bf16)
        k.send(0)

    def relay1(c):
        k = Chunk(c)
        k.received(0)
        got, buf = recv_bufs[0], send_bufs[1]
        buf[k.slot, 0] = (k.term(1, 0) + got[k.slot, 0, :half1].astype(f32)).astype(bf16)
        buf[k.slot, 1] = (k.term(-1, 1) + got[k.slot, 1, half1:].astype(f32)).astype(bf16)
        k.send(1)
        part[k.slot, :half1] = k.term(0, 0) + got[k.slot, 1, :half1].astype(f32)
        part[k.slot, half1:] = k.term(0, 1) + got[k.slot, 0, half1:].astype(f32)

    def shard1(c):
        k = Chunk(c)
        k.received(1)
        got = recv_bufs[1]
        part[k.slot, :half1] += got[k.slot, 0].astype(f32)
        part[k.slot, half1:] += got[k.slot, 1].astype(f32)
        buf = send_bufs[2]
        buf[k.slot, 0, :half2] = k.sub(2, 0).astype(bf16)
        buf[k.slot, 0, half2:] = k.sub(1, 1).astype(bf16)
        buf[k.slot, 1, :half2] = k.sub(-1, 0).astype(bf16)
        buf[k.slot, 1, half2:] = k.sub(2, 1).astype(bf16)
        k.send(2)

    def relay2(c):
        k = Chunk(c)
        k.received(2)
        got, buf = recv_bufs[2], send_bufs[3]
        buf[k.slot, 0] = (k.sub(1, 0) + got[k.slot, 0, :half2].astype(f32)).astype(bf16)
        buf[k.slot, 1] = (k.sub(-1, 1) + got[k.slot, 1, half2:].astype(f32)).astype(bf16)
        k.send(3)
        mine[k.slot, :half2] = k.sub(0, 0) + got[k.slot, 1, :half2].astype(f32)
        mine[k.slot, half2:] = k.sub(0, 1) + got[k.slot, 0, half2:].astype(f32)

    def shard2(c):
        k = Chunk(c)
        k.received(3)
        got = recv_bufs[3]
        low = mine[k.slot, :half2] + got[k.slot, 0].astype(f32)
        high = mine[k.slot, half2:] + got[k.slot, 1].astype(f32)
        k.block(0, k.q * rows2, half2)[...] = low.astype(bf16)
        k.block(0, k.q * rows2 + half2, half2)[...] = high.astype(bf16)
        k.send(4)

    def gather2(c):
        k = Chunk(c)
        k.received(4)
        k.send(5)

    def gathered2(c):
        Chunk(c).received(5)

    def gather1(c):
        Chunk(c).send(6)

    def relay_gather1(c):
        k = Chunk(c)
        k.received(6)
        k.send(7)

    def gathered1(c):
        Chunk(c).received(7)

    sends = [0, 1, 2, 3, 4, 5, 6 + HOLD, 7 + HOLD]
    steps = list(zip(sends, (multiply, relay1, shard1, relay2, shard2, gather2, gather1, relay_gather1)))
    steps += [(6, gathered2), (8 + HOLD, gathered1)]
    steps.sort(key=lambda step: step[0])
    for stage, lag in enumerate(sends):
        steps.append((lag + 2, functools.partial(lambda stage, c: Chunk(c).sent(stage), stage)))

    barrier = pltpu.get_barrier_semaphore()
    here = Chunk(0)
    for copy in (*a_copies(0), *g_copies(0), *g_copies(1)):
        copy.start()
    for to in (1, -1):
        for device in (here.first(to), here.second(to)):
            pl.semaphore_signal(barrier, inc=1, device_id={"dp": device}, device_id_type=pl.DeviceIdType.MESH)
    pl.semaphore_wait(barrier, 4)

    def turn(t, carry):
        for lag, do in steps:
            @pl.when((t >= lag) & (t < lag + chunks))
            def _(lag=lag, do=do):
                do(t - lag)
        return carry

    lax.fori_loop(0, chunks + max(lag for lag, _ in steps), turn, 0)


def write(sums, out, sem):
    matrices, rows = sums.shape[:2]
    size = rows // PIECES
    copies = [
        pltpu.make_async_copy(
            sums.at[n, i * size : (i + 1) * size], out.at[n, i * size : (i + 1) * size], sem.at[n, i]
        )
        for n in range(matrices)
        for i in range(PIECES)
    ]
    for copy in copies:
        copy.start()
    for copy in copies:
        copy.wait()


def solution(mesh):
    side = math.isqrt(mesh.shape["dp"])

    def body(a, g):
        matrices, tokens, rows = a.shape[1:]
        columns = g.shape[3]
        width = side * LANES
        sizes = (rows, rows // 2, rows // side, rows // side // 2)
        messages = [pltpu.VMEM((SLOTS, 2, size, LANES), jnp.bfloat16) for size in sizes]
        sums = pl.pallas_call(
            functools.partial(kernel, side),
            name="gradient_sums",
            out_shape=pltpu.VMEM((matrices, rows, columns), jnp.bfloat16),
            in_specs=[pl.BlockSpec(memory_space=pl.ANY)] * 2,
            out_specs=pl.BlockSpec(memory_space=pltpu.VMEM),
            scratch_shapes=[
                pltpu.VMEM((2, tokens, rows), jnp.bfloat16),
                pltpu.VMEM((G_SLOTS, tokens, width), jnp.bfloat16),
                pltpu.VMEM((2, rows, width), jnp.float32),
                pltpu.VMEM((SLOTS, rows, LANES), jnp.float32),
                pltpu.VMEM((SLOTS, rows // side, LANES), jnp.float32),
                *messages,
                *messages,
                pltpu.SemaphoreType.DMA((2, PIECES)),
                pltpu.SemaphoreType.DMA((G_SLOTS, PIECES)),
                pltpu.SemaphoreType.DMA((8, 2, SLOTS)),
                pltpu.SemaphoreType.DMA((8, 2, SLOTS)),
            ],
            compiler_params=pltpu.CompilerParams(
                collective_id=0, has_side_effects=True, vmem_limit_bytes=50 << 20
            ),
        )(a, g)
        return pl.pallas_call(
            write,
            name="write_sums",
            out_shape=jax.ShapeDtypeStruct(sums.shape, sums.dtype),
            in_specs=[pl.BlockSpec(memory_space=pltpu.VMEM)],
            out_specs=pl.BlockSpec(memory_space=pl.ANY),
            scratch_shapes=[pltpu.SemaphoreType.DMA((matrices, PIECES))],
            compiler_params=pltpu.CompilerParams(vmem_limit_bytes=1 << 20),
        )(sums)

    spec = P(("rep", "dp"), None, None, None)
    return jax.shard_map(body, mesh=mesh, in_specs=(spec, spec), out_specs=P("rep", None, None), check_vma=False)
```

```python
import functools
import math

import jax
import jax.numpy as jnp
from jax import lax
from jax.experimental import pallas as pl
from jax.experimental.pallas import tpu as pltpu
from jax.sharding import PartitionSpec as P

LANES = 128
SLOTS = 4
SEMS = 8
PIECES = 4
G_SLOTS = 3


def kernel(side, a_hbm, g_hbm, out, a_buf, g_buf, acc, part, mine, *rest):
    send_bufs, recv_bufs = rest[:4], rest[4:8]
    a_sem, g_sem, send_sem, recv_sem = rest[8:]
    matrices, tokens, rows = a_hbm.shape[1:]
    width = side * LANES
    per_matrix = g_hbm.shape[3] // width
    chunks = matrices * per_matrix
    half1, rows2 = rows // 2, rows // side
    half2 = rows2 // 2
    me, swap = lax.axis_index("dp"), lax.axis_index("rep") % 2
    x, y = me // side, me % side
    bf16, f32 = jnp.bfloat16, jnp.float32

    class Chunk:
        def __init__(self, c):
            odd = (c + swap) % 2
            self.c, self.slot, self.sem = c, c % SLOTS, c % SEMS
            self.matrix = c // per_matrix
            self.column = (c % per_matrix) * width
            self.p = x * (1 - odd) + y * odd
            self.q = y * (1 - odd) + x * odd
            self.stride1 = side * (1 - odd) + odd
            self.stride2 = side * odd + 1 - odd

        def first(self, d):
            return (self.p + d + side) % side * self.stride1 + self.q * self.stride2

        def second(self, d):
            return self.p * self.stride1 + (self.q + d + side) % side * self.stride2

        def term(self, d, half):
            s = (self.p + d + side) % side
            lanes = pl.ds(pl.multiple_of(s * LANES, LANES), LANES)
            return acc[self.c % 2, half * half1 : (half + 1) * half1, lanes]

        def sub(self, d, half):
            s = (self.q + d + side) % side
            return part[self.slot, pl.ds(pl.multiple_of(s * rows2 + half * half2, half2), half2), :]

        def block(self, d1, start, size):
            s = (self.p + d1 + side) % side
            lanes = pl.ds(pl.multiple_of(self.column + s * LANES, LANES), LANES)
            return out.at[self.matrix, pl.ds(pl.multiple_of(start, 16), size), lanes]

        def copy(self, stage, way):
            to = 1 - 2 * way
            if stage < 4:
                src, dst = send_bufs[stage].at[self.slot, way], recv_bufs[stage].at[self.slot, way]
                device = self.first(to) if stage < 2 else self.second(to)
            elif stage == 4:
                src = dst = self.block(0, self.q * rows2, rows2)
                device = self.second(to)
            elif stage == 5:
                src = dst = self.block(0, (self.q - to + side) % side * rows2 + way * half2, half2)
                device = self.second(to)
            elif stage == 6:
                src = dst = self.block(0, 0, rows)
                device = self.first(to)
            else:
                src = dst = self.block(-to, way * half1, half1)
                device = self.first(to)
            return pltpu.make_async_remote_copy(
                src_ref=src,
                dst_ref=dst,
                send_sem=send_sem.at[stage, way, self.sem],
                recv_sem=recv_sem.at[stage, way, self.sem],
                device_id={"dp": device},
                device_id_type=pl.DeviceIdType.MESH,
            )

        def send(self, stage):
            for way in range(2):
                self.copy(stage, way).start()

        def received(self, stage):
            for way in range(2):
                self.copy(stage, way).wait_recv()

        def sent(self, stage):
            for way in range(2):
                self.copy(stage, way).wait_send()

    def a_copies(n):
        depth = tokens // PIECES
        for i in range(PIECES):
            piece = pl.ds(i * depth, depth)
            yield pltpu.make_async_copy(a_hbm.at[0, n, piece, :], a_buf.at[n % 2, piece, :], a_sem.at[n % 2, i])

    def g_copies(c):
        depth = tokens // PIECES
        lanes = pl.ds(pl.multiple_of(c % per_matrix * width, width), width)
        for i in range(PIECES):
            piece = pl.ds(i * depth, depth)
            yield pltpu.make_async_copy(
                g_hbm.at[0, c // per_matrix, piece, lanes], g_buf.at[c % G_SLOTS, piece, :], g_sem.at[c % G_SLOTS, i]
            )

    def product(n, c, tokens):
        return lax.dot_general(
            a_buf[n % 2, tokens, :], g_buf[c % G_SLOTS, tokens, :], (((0,), (0,)), ((), ())), preferred_element_type=f32
        )

    def start(copies):
        for copy in copies:
            copy.start()

    def wait(copies):
        for copy in copies:
            copy.wait()

    def multiply(c):
        k = Chunk(c)

        @pl.when(c == 0)
        def _():
            depth = tokens // PIECES
            pieces = list(zip(a_copies(0), g_copies(0)))
            for i in range(PIECES):
                wait(pieces[i])
                if i + 2 < PIECES:
                    start(pieces[i + 2])
                elif i + 2 == PIECES:
                    start(g_copies(1))
                term = product(0, 0, slice(i * depth, (i + 1) * depth))
                acc[0] = term if i == 0 else acc[0] + term

        @pl.when(c > 0)
        def _():
            @pl.when(c % per_matrix == 0)
            def _():
                wait(a_copies(k.matrix))

            wait(g_copies(c))
            acc[c % 2] = product(k.matrix, c, slice(None))

        @pl.when((c % per_matrix == 0) & (k.matrix + 1 < matrices))
        def _():
            start(a_copies(k.matrix + 1))

        @pl.when(c + 2 < chunks)
        def _():
            start(g_copies(c + 2))

        buf = send_bufs[0]
        buf[k.slot, 0, :half1] = k.term(2, 0).astype(bf16)
        buf[k.slot, 0, half1:] = k.term(1, 1).astype(bf16)
        buf[k.slot, 1, :half1] = k.term(-1, 0).astype(bf16)
        buf[k.slot, 1, half1:] = k.term(2, 1).astype(bf16)
        k.send(0)

    def relay1(c):
        k = Chunk(c)
        k.received(0)
        got, buf = recv_bufs[0], send_bufs[1]
        buf[k.slot, 0] = (k.term(1, 0) + got[k.slot, 0, :half1].astype(f32)).astype(bf16)
        buf[k.slot, 1] = (k.term(-1, 1) + got[k.slot, 1, half1:].astype(f32)).astype(bf16)
        k.send(1)
        part[k.slot, :half1] = k.term(0, 0) + got[k.slot, 1, :half1].astype(f32)
        part[k.slot, half1:] = k.term(0, 1) + got[k.slot, 0, half1:].astype(f32)

    def shard1(c):
        k = Chunk(c)
        k.received(1)
        got = recv_bufs[1]
        part[k.slot, :half1] += got[k.slot, 0].astype(f32)
        part[k.slot, half1:] += got[k.slot, 1].astype(f32)
        buf = send_bufs[2]
        buf[k.slot, 0, :half2] = k.sub(2, 0).astype(bf16)
        buf[k.slot, 0, half2:] = k.sub(1, 1).astype(bf16)
        buf[k.slot, 1, :half2] = k.sub(-1, 0).astype(bf16)
        buf[k.slot, 1, half2:] = k.sub(2, 1).astype(bf16)
        k.send(2)

    def relay2(c):
        k = Chunk(c)
        k.received(2)
        got, buf = recv_bufs[2], send_bufs[3]
        buf[k.slot, 0] = (k.sub(1, 0) + got[k.slot, 0, :half2].astype(f32)).astype(bf16)
        buf[k.slot, 1] = (k.sub(-1, 1) + got[k.slot, 1, half2:].astype(f32)).astype(bf16)
        k.send(3)
        mine[k.slot, :half2] = k.sub(0, 0) + got[k.slot, 1, :half2].astype(f32)
        mine[k.slot, half2:] = k.sub(0, 1) + got[k.slot, 0, half2:].astype(f32)

    def shard2(c):
        k = Chunk(c)
        k.received(3)
        got = recv_bufs[3]
        low = mine[k.slot, :half2] + got[k.slot, 0].astype(f32)
        high = mine[k.slot, half2:] + got[k.slot, 1].astype(f32)
        k.block(0, k.q * rows2, half2)[...] = low.astype(bf16)
        k.block(0, k.q * rows2 + half2, half2)[...] = high.astype(bf16)
        k.send(4)

    def gather2(c):
        k = Chunk(c)
        k.received(4)
        k.send(5)

    def gathered2(c):
        Chunk(c).received(5)

    def gather1(c):
        Chunk(c).send(6)

    def relay_gather1(c):
        k = Chunk(c)
        k.received(6)
        k.send(7)

    def gathered1(c):
        Chunk(c).received(7)

    sends = [0, 1, 2, 3, 4, 5, 6, 9]
    steps = list(zip(sends, (multiply, relay1, shard1, relay2, shard2, gather2)))
    steps += [(6, gathered2), (sends[6], gather1), (sends[7], relay_gather1), (12, gathered1)]
    for stage, lag in enumerate(sends):
        steps.append((lag + 3, functools.partial(lambda stage, c: Chunk(c).sent(stage), stage)))

    barrier = pltpu.get_barrier_semaphore()
    here = Chunk(0)
    for pair in list(zip(a_copies(0), g_copies(0)))[:2]:
        start(pair)
    for to in (1, -1):
        for device in (here.first(to), here.second(to)):
            pl.semaphore_signal(barrier, inc=1, device_id={"dp": device}, device_id_type=pl.DeviceIdType.MESH)
    pl.semaphore_wait(barrier, 4)

    def turn(t, carry):
        for lag, do in steps:
            @pl.when((t >= lag) & (t < lag + chunks))
            def _(lag=lag, do=do):
                do(t - lag)
        return carry

    lax.fori_loop(0, chunks + max(lag for lag, _ in steps), turn, 0)


def write(sums, out, sem):
    matrices, rows = sums.shape[:2]
    size = rows // PIECES
    copies = [
        pltpu.make_async_copy(
            sums.at[n, i * size : (i + 1) * size], out.at[n, i * size : (i + 1) * size], sem.at[n, i]
        )
        for n in range(matrices)
        for i in range(PIECES)
    ]
    for copy in copies:
        copy.start()
    for copy in copies:
        copy.wait()


def solution(mesh):
    side = math.isqrt(mesh.shape["dp"])

    def body(a, g):
        matrices, tokens, rows = a.shape[1:]
        columns = g.shape[3]
        width = side * LANES
        sizes = (rows, rows // 2, rows // side, rows // side // 2)
        messages = [pltpu.VMEM((SLOTS, 2, size, LANES), jnp.bfloat16) for size in sizes]
        sums = pl.pallas_call(
            functools.partial(kernel, side),
            name="gradient_sums",
            out_shape=pltpu.VMEM((matrices, rows, columns), jnp.bfloat16),
            in_specs=[pl.BlockSpec(memory_space=pl.ANY)] * 2,
            out_specs=pl.BlockSpec(memory_space=pltpu.VMEM),
            scratch_shapes=[
                pltpu.VMEM((2, tokens, rows), jnp.bfloat16),
                pltpu.VMEM((G_SLOTS, tokens, width), jnp.bfloat16),
                pltpu.VMEM((2, rows, width), jnp.float32),
                pltpu.VMEM((SLOTS, rows, LANES), jnp.float32),
                pltpu.VMEM((SLOTS, rows // side, LANES), jnp.float32),
                *messages,
                *messages,
                pltpu.SemaphoreType.DMA((2, PIECES)),
                pltpu.SemaphoreType.DMA((G_SLOTS, PIECES)),
                pltpu.SemaphoreType.DMA((8, 2, SEMS)),
                pltpu.SemaphoreType.DMA((8, 2, SEMS)),
            ],
            compiler_params=pltpu.CompilerParams(
                collective_id=0, has_side_effects=True, vmem_limit_bytes=50 << 20
            ),
        )(a, g)
        return pl.pallas_call(
            write,
            name="write_sums",
            out_shape=jax.ShapeDtypeStruct(sums.shape, sums.dtype),
            in_specs=[pl.BlockSpec(memory_space=pltpu.VMEM)],
            out_specs=pl.BlockSpec(memory_space=pl.ANY),
            scratch_shapes=[pltpu.SemaphoreType.DMA((matrices, PIECES))],
            compiler_params=pltpu.CompilerParams(vmem_limit_bytes=1 << 20),
        )(sums)

    spec = P(("rep", "dp"), None, None, None)
    return jax.shard_map(body, mesh=mesh, in_specs=(spec, spec), out_specs=P("rep", None, None), check_vma=False)
```

```python
import functools
import math

import jax
import jax.numpy as jnp
from jax import lax
from jax.experimental import pallas as pl
from jax.experimental.pallas import tpu as pltpu
from jax.sharding import PartitionSpec as P

LANES = 128
SEND_SLOTS = 4
RECV_SLOTS = 8
ACC_SLOTS = 4
PIECES = 4
G_SLOTS = 3


def kernel(side, a_hbm, g_hbm, out, a_buf, g_buf, acc, part, mine, *rest):
    send_bufs, recv_bufs = rest[:4], rest[4:8]
    a_sem, g_sem, send_sem, recv_sem = rest[8:]
    matrices, tokens, rows = a_hbm.shape[1:]
    width = side * LANES
    per_matrix = g_hbm.shape[3] // width
    chunks = matrices * per_matrix
    half1, rows2 = rows // 2, rows // side
    half2 = rows2 // 2
    me, swap = lax.axis_index("dp"), lax.axis_index("rep") % 2
    x, y = me // side, me % side
    bf16, f32 = jnp.bfloat16, jnp.float32

    class Chunk:
        def __init__(self, c):
            odd = (c + swap) % 2
            self.c, self.slot, self.recv = c, c % SEND_SLOTS, c % RECV_SLOTS
            self.matrix = c // per_matrix
            self.column = (c % per_matrix) * width
            self.p = x * (1 - odd) + y * odd
            self.q = y * (1 - odd) + x * odd
            self.stride1 = side * (1 - odd) + odd
            self.stride2 = side * odd + 1 - odd

        def first(self, d):
            return (self.p + d + side) % side * self.stride1 + self.q * self.stride2

        def second(self, d):
            return self.p * self.stride1 + (self.q + d + side) % side * self.stride2

        def term(self, d, half):
            s = (self.p + d + side) % side
            lanes = pl.ds(pl.multiple_of(s * LANES, LANES), LANES)
            return acc[self.c % ACC_SLOTS, half * half1 : (half + 1) * half1, lanes]

        def sub(self, d, half):
            s = (self.q + d + side) % side
            return part[self.recv, pl.ds(pl.multiple_of(s * rows2 + half * half2, half2), half2), :]

        def block(self, d1, start, size):
            s = (self.p + d1 + side) % side
            lanes = pl.ds(pl.multiple_of(self.column + s * LANES, LANES), LANES)
            return out.at[self.matrix, pl.ds(pl.multiple_of(start, 16), size), lanes]

        def copy(self, stage, way):
            to = 1 - 2 * way
            if stage < 4:
                src, dst = send_bufs[stage].at[self.slot, way], recv_bufs[stage].at[self.recv, way]
                device = self.first(to) if stage < 2 else self.second(to)
            elif stage == 4:
                src = dst = self.block(0, self.q * rows2, rows2)
                device = self.second(to)
            elif stage == 5:
                src = dst = self.block(0, (self.q - to + side) % side * rows2 + way * half2, half2)
                device = self.second(to)
            elif stage == 6:
                src = dst = self.block(0, 0, rows)
                device = self.first(to)
            else:
                src = dst = self.block(-to, way * half1, half1)
                device = self.first(to)
            return pltpu.make_async_remote_copy(
                src_ref=src,
                dst_ref=dst,
                send_sem=send_sem.at[stage, way, self.recv],
                recv_sem=recv_sem.at[stage, way, self.recv],
                device_id={"dp": device},
                device_id_type=pl.DeviceIdType.MESH,
            )

        def send(self, stage):
            for way in range(2):
                self.copy(stage, way).start()

        def received(self, stage):
            for way in range(2):
                self.copy(stage, way).wait_recv()

        def sent(self, stage):
            for way in range(2):
                self.copy(stage, way).wait_send()

    def a_copies(n):
        depth = tokens // PIECES
        for i in range(PIECES):
            piece = pl.ds(i * depth, depth)
            yield pltpu.make_async_copy(a_hbm.at[0, n, piece, :], a_buf.at[n % 2, piece, :], a_sem.at[n % 2, i])

    def g_copies(c):
        depth = tokens // PIECES
        lanes = pl.ds(pl.multiple_of(c % per_matrix * width, width), width)
        for i in range(PIECES):
            piece = pl.ds(i * depth, depth)
            yield pltpu.make_async_copy(
                g_hbm.at[0, c // per_matrix, piece, lanes], g_buf.at[c % G_SLOTS, piece, :], g_sem.at[c % G_SLOTS, i]
            )

    def product(n, c, tokens):
        return lax.dot_general(
            a_buf[n % 2, tokens, :], g_buf[c % G_SLOTS, tokens, :], (((0,), (0,)), ((), ())), preferred_element_type=f32
        )

    def start(copies):
        for copy in copies:
            copy.start()

    def wait(copies):
        for copy in copies:
            copy.wait()

    def multiply(c):
        k = Chunk(c)

        @pl.when(c == 0)
        def _():
            depth = tokens // PIECES
            pieces = list(zip(a_copies(0), g_copies(0)))
            for i in range(PIECES):
                wait(pieces[i])
                if i + 2 < PIECES:
                    start(pieces[i + 2])
                elif i + 2 == PIECES:
                    start(g_copies(1))
                term = product(0, 0, slice(i * depth, (i + 1) * depth))
                acc[0] = term if i == 0 else acc[0] + term

        @pl.when(c > 0)
        def _():
            @pl.when(c % per_matrix == 0)
            def _():
                wait(a_copies(k.matrix))

            wait(g_copies(c))
            acc[c % ACC_SLOTS] = product(k.matrix, c, slice(None))

        @pl.when((c % per_matrix == 0) & (k.matrix + 1 < matrices))
        def _():
            start(a_copies(k.matrix + 1))

        @pl.when(c + 2 < chunks)
        def _():
            start(g_copies(c + 2))

        buf = send_bufs[0]
        buf[k.slot, 0, :half1] = k.term(2, 0).astype(bf16)
        buf[k.slot, 0, half1:] = k.term(1, 1).astype(bf16)
        buf[k.slot, 1, :half1] = k.term(-1, 0).astype(bf16)
        buf[k.slot, 1, half1:] = k.term(2, 1).astype(bf16)
        k.send(0)

    def relay1(c):
        k = Chunk(c)
        k.received(0)
        got, buf = recv_bufs[0], send_bufs[1]
        buf[k.slot, 0] = (k.term(1, 0) + got[k.recv, 0, :half1].astype(f32)).astype(bf16)
        buf[k.slot, 1] = (k.term(-1, 1) + got[k.recv, 1, half1:].astype(f32)).astype(bf16)
        k.send(1)
        part[k.recv, :half1] = k.term(0, 0) + got[k.recv, 1, :half1].astype(f32)
        part[k.recv, half1:] = k.term(0, 1) + got[k.recv, 0, half1:].astype(f32)

    def shard1(c):
        k = Chunk(c)
        k.received(1)
        got = recv_bufs[1]
        part[k.recv, :half1] += got[k.recv, 0].astype(f32)
        part[k.recv, half1:] += got[k.recv, 1].astype(f32)
        buf = send_bufs[2]
        buf[k.slot, 0, :half2] = k.sub(2, 0).astype(bf16)
        buf[k.slot, 0, half2:] = k.sub(1, 1).astype(bf16)
        buf[k.slot, 1, :half2] = k.sub(-1, 0).astype(bf16)
        buf[k.slot, 1, half2:] = k.sub(2, 1).astype(bf16)
        k.send(2)

    def relay2(c):
        k = Chunk(c)
        k.received(2)
        got, buf = recv_bufs[2], send_bufs[3]
        buf[k.slot, 0] = (k.sub(1, 0) + got[k.recv, 0, :half2].astype(f32)).astype(bf16)
        buf[k.slot, 1] = (k.sub(-1, 1) + got[k.recv, 1, half2:].astype(f32)).astype(bf16)
        k.send(3)
        mine[k.slot, :half2] = k.sub(0, 0) + got[k.recv, 1, :half2].astype(f32)
        mine[k.slot, half2:] = k.sub(0, 1) + got[k.recv, 0, half2:].astype(f32)

    def shard2(c):
        k = Chunk(c)
        k.received(3)
        got = recv_bufs[3]
        low = mine[k.slot, :half2] + got[k.recv, 0].astype(f32)
        high = mine[k.slot, half2:] + got[k.recv, 1].astype(f32)
        k.block(0, k.q * rows2, half2)[...] = low.astype(bf16)
        k.block(0, k.q * rows2 + half2, half2)[...] = high.astype(bf16)
        k.send(4)

    def gather2(c):
        k = Chunk(c)
        k.received(4)
        k.send(5)

    def gathered2(c):
        Chunk(c).received(5)

    def gather1(c):
        Chunk(c).send(6)

    def relay_gather1(c):
        k = Chunk(c)
        k.received(6)
        k.send(7)

    def gathered1(c):
        Chunk(c).received(7)

    sends = [0, 2, 4, 6, 8, 10, 12, 15]
    steps = list(zip(sends, (multiply, relay1, shard1, relay2, shard2, gather2)))
    steps += [(12, gathered2), (sends[6], gather1), (sends[7], relay_gather1), (18, gathered1)]
    for stage, lag in enumerate(sends):
        steps.append((lag + 3, functools.partial(lambda stage, c: Chunk(c).sent(stage), stage)))

    barrier = pltpu.get_barrier_semaphore()
    here = Chunk(0)
    for pair in list(zip(a_copies(0), g_copies(0)))[:2]:
        start(pair)
    for to in (1, -1):
        for device in (here.first(to), here.second(to)):
            pl.semaphore_signal(barrier, inc=1, device_id={"dp": device}, device_id_type=pl.DeviceIdType.MESH)
    pl.semaphore_wait(barrier, 4)

    def turn(t, carry):
        for lag, do in steps:
            @pl.when((t >= lag) & (t < lag + chunks))
            def _(lag=lag, do=do):
                do(t - lag)
        return carry

    lax.fori_loop(0, chunks + max(lag for lag, _ in steps), turn, 0)


def write(sums, out, sem):
    matrices, rows = sums.shape[:2]
    size = rows // PIECES
    copies = [
        pltpu.make_async_copy(
            sums.at[n, i * size : (i + 1) * size], out.at[n, i * size : (i + 1) * size], sem.at[n, i]
        )
        for n in range(matrices)
        for i in range(PIECES)
    ]
    for copy in copies:
        copy.start()
    for copy in copies:
        copy.wait()


def solution(mesh):
    side = math.isqrt(mesh.shape["dp"])

    def body(a, g):
        matrices, tokens, rows = a.shape[1:]
        columns = g.shape[3]
        width = side * LANES
        sizes = (rows, rows // 2, rows // side, rows // side // 2)
        messages = [
            pltpu.VMEM((slots, 2, size, LANES), jnp.bfloat16) for slots in (SEND_SLOTS, RECV_SLOTS) for size in sizes
        ]
        sums = pl.pallas_call(
            functools.partial(kernel, side),
            name="gradient_sums",
            out_shape=pltpu.VMEM((matrices, rows, columns), jnp.bfloat16),
            in_specs=[pl.BlockSpec(memory_space=pl.ANY)] * 2,
            out_specs=pl.BlockSpec(memory_space=pltpu.VMEM),
            scratch_shapes=[
                pltpu.VMEM((2, tokens, rows), jnp.bfloat16),
                pltpu.VMEM((G_SLOTS, tokens, width), jnp.bfloat16),
                pltpu.VMEM((ACC_SLOTS, rows, width), jnp.float32),
                pltpu.VMEM((RECV_SLOTS, rows, LANES), jnp.float32),
                pltpu.VMEM((SEND_SLOTS, rows // side, LANES), jnp.float32),
                *messages,
                pltpu.SemaphoreType.DMA((2, PIECES)),
                pltpu.SemaphoreType.DMA((G_SLOTS, PIECES)),
                pltpu.SemaphoreType.DMA((8, 2, RECV_SLOTS)),
                pltpu.SemaphoreType.DMA((8, 2, RECV_SLOTS)),
            ],
            compiler_params=pltpu.CompilerParams(
                collective_id=0, has_side_effects=True, vmem_limit_bytes=50 << 20
            ),
        )(a, g)
        return pl.pallas_call(
            write,
            name="write_sums",
            out_shape=jax.ShapeDtypeStruct(sums.shape, sums.dtype),
            in_specs=[pl.BlockSpec(memory_space=pltpu.VMEM)],
            out_specs=pl.BlockSpec(memory_space=pl.ANY),
            scratch_shapes=[pltpu.SemaphoreType.DMA((matrices, PIECES))],
            compiler_params=pltpu.CompilerParams(vmem_limit_bytes=1 << 20),
        )(sums)

    spec = P(("rep", "dp"), None, None, None)
    return jax.shard_map(body, mesh=mesh, in_specs=(spec, spec), out_specs=P("rep", None, None), check_vma=False)
```

```python
import functools
import math

import jax
import jax.numpy as jnp
from jax import lax
from jax.experimental import pallas as pl
from jax.experimental.pallas import tpu as pltpu
from jax.sharding import PartitionSpec as P

LANES = 128
SEND_SLOTS = 4
RECV_SLOTS = 8
PIECES = 4
G_SLOTS = 3


def kernel(side, a_hbm, g_hbm, out, a_buf, g_buf, total, acc, part, mine, *rest):
    send_bufs, recv_bufs = rest[:4], rest[4:8]
    a_sem, g_sem, send_sem, recv_sem = rest[8:]
    matrices, tokens, rows = a_hbm.shape[1:]
    width = side * LANES
    per_matrix = g_hbm.shape[3] // width
    chunks = matrices * per_matrix
    half1, rows2 = rows // 2, rows // side
    half2 = rows2 // 2
    me, swap = lax.axis_index("dp"), lax.axis_index("rep") % 2
    x, y = me // side, me % side
    bf16, f32 = jnp.bfloat16, jnp.float32

    class Chunk:
        def __init__(self, c):
            odd = (c + swap) % 2
            self.c, self.slot, self.recv = c, c % SEND_SLOTS, c % RECV_SLOTS
            self.matrix = c // per_matrix
            self.column = (c % per_matrix) * side
            self.p = x * (1 - odd) + y * odd
            self.q = y * (1 - odd) + x * odd
            self.stride1 = side * (1 - odd) + odd
            self.stride2 = side * odd + 1 - odd

        def first(self, d):
            return (self.p + d + side) % side * self.stride1 + self.q * self.stride2

        def second(self, d):
            return self.p * self.stride1 + (self.q + d + side) % side * self.stride2

        def lanes(self, d):
            return pl.ds(pl.multiple_of((self.p + d + side) % side * LANES, LANES), LANES)

        def sub(self, d, half):
            s = (self.q + d + side) % side
            return part[self.recv, pl.ds(pl.multiple_of(s * rows2 + half * half2, half2), half2), :]

        def block(self, d1, start, size):
            s = (self.p + d1 + side) % side
            return out.at[self.matrix, self.column + s, pl.ds(pl.multiple_of(start, 16), size), :]

        def copy(self, stage, way):
            to = 1 - 2 * way
            if stage < 4:
                src, dst = send_bufs[stage].at[self.slot, way], recv_bufs[stage].at[self.recv, way]
                device = self.first(to) if stage < 2 else self.second(to)
            elif stage == 4:
                src = dst = self.block(0, self.q * rows2, rows2)
                device = self.second(to)
            elif stage == 5:
                src = dst = self.block(0, (self.q - to + side) % side * rows2 + way * half2, half2)
                device = self.second(to)
            elif stage == 6:
                src = dst = self.block(0, 0, rows)
                device = self.first(to)
            else:
                src = dst = self.block(-to, way * half1, half1)
                device = self.first(to)
            return pltpu.make_async_remote_copy(
                src_ref=src,
                dst_ref=dst,
                send_sem=send_sem.at[stage, way, self.recv],
                recv_sem=recv_sem.at[stage, way, self.recv],
                device_id={"dp": device},
                device_id_type=pl.DeviceIdType.MESH,
            )

        def send(self, stage):
            for way in range(2):
                self.copy(stage, way).start()

        def received(self, stage):
            for way in range(2):
                self.copy(stage, way).wait_recv()

        def sent(self, stage):
            for way in range(2):
                self.copy(stage, way).wait_send()

    def a_copies(n):
        depth = tokens // PIECES
        for i in range(PIECES):
            piece = pl.ds(i * depth, depth)
            yield pltpu.make_async_copy(a_hbm.at[0, n, piece, :], a_buf.at[n % 2, piece, :], a_sem.at[n % 2, i])

    def g_copies(c):
        depth = tokens // PIECES
        lanes = pl.ds(pl.multiple_of(c % per_matrix * width, width), width)
        for i in range(PIECES):
            piece = pl.ds(i * depth, depth)
            yield pltpu.make_async_copy(
                g_hbm.at[0, c // per_matrix, piece, lanes], g_buf.at[c % G_SLOTS, piece, :], g_sem.at[c % G_SLOTS, i]
            )

    def product(k, tokens):
        g = g_buf.at[k.c % G_SLOTS]
        columns = jnp.concatenate([g[tokens, k.lanes(d)] for d in (1, 2, -1, 0)], axis=1)
        return lax.dot_general(
            a_buf[k.matrix % 2, tokens, :], columns, (((0,), (0,)), ((), ())), preferred_element_type=f32
        )

    def store(k, product):
        right, far, left, own = (product[:, i * LANES : (i + 1) * LANES] for i in range(4))
        buf = send_bufs[0]
        buf[k.slot, 0, :half1] = far[:half1].astype(bf16)
        buf[k.slot, 0, half1:] = right[half1:].astype(bf16)
        buf[k.slot, 1, :half1] = left[:half1].astype(bf16)
        buf[k.slot, 1, half1:] = far[half1:].astype(bf16)
        acc[k.slot, 0] = right[:half1]
        acc[k.slot, 1] = left[half1:]
        part[k.recv] = own

    def start(copies):
        for copy in copies:
            copy.start()

    def wait(copies):
        for copy in copies:
            copy.wait()

    def multiply(c):
        k = Chunk(c)

        @pl.when(c == 0)
        def _():
            depth = tokens // PIECES
            pieces = list(zip(a_copies(0), g_copies(0)))
            for i in range(PIECES):
                wait(pieces[i])
                if i + 2 < PIECES:
                    start(pieces[i + 2])
                elif i + 2 == PIECES:
                    start(g_copies(1))
                term = product(k, slice(i * depth, (i + 1) * depth))
                if i == 0:
                    total[...] = term
                elif i + 1 < PIECES:
                    total[...] += term
                else:
                    store(k, total[...] + term)

        @pl.when(c > 0)
        def _():
            @pl.when(c % per_matrix == 0)
            def _():
                wait(a_copies(k.matrix))

            wait(g_copies(c))
            store(k, product(k, slice(None)))

        @pl.when((c % per_matrix == 0) & (k.matrix + 1 < matrices))
        def _():
            start(a_copies(k.matrix + 1))

        @pl.when(c + 2 < chunks)
        def _():
            start(g_copies(c + 2))

        k.send(0)

    def relay1(c):
        k = Chunk(c)
        k.received(0)
        got, buf = recv_bufs[0], send_bufs[1]
        buf[k.slot, 0] = (acc[k.slot, 0] + got[k.recv, 0, :half1].astype(f32)).astype(bf16)
        buf[k.slot, 1] = (acc[k.slot, 1] + got[k.recv, 1, half1:].astype(f32)).astype(bf16)
        k.send(1)
        part[k.recv, :half1] += got[k.recv, 1, :half1].astype(f32)
        part[k.recv, half1:] += got[k.recv, 0, half1:].astype(f32)

    def shard1(c):
        k = Chunk(c)
        k.received(1)
        got = recv_bufs[1]
        part[k.recv, :half1] += got[k.recv, 0].astype(f32)
        part[k.recv, half1:] += got[k.recv, 1].astype(f32)
        buf = send_bufs[2]
        buf[k.slot, 0, :half2] = k.sub(2, 0).astype(bf16)
        buf[k.slot, 0, half2:] = k.sub(1, 1).astype(bf16)
        buf[k.slot, 1, :half2] = k.sub(-1, 0).astype(bf16)
        buf[k.slot, 1, half2:] = k.sub(2, 1).astype(bf16)
        k.send(2)

    def relay2(c):
        k = Chunk(c)
        k.received(2)
        got, buf = recv_bufs[2], send_bufs[3]
        buf[k.slot, 0] = (k.sub(1, 0) + got[k.recv, 0, :half2].astype(f32)).astype(bf16)
        buf[k.slot, 1] = (k.sub(-1, 1) + got[k.recv, 1, half2:].astype(f32)).astype(bf16)
        k.send(3)
        mine[k.slot, :half2] = k.sub(0, 0) + got[k.recv, 1, :half2].astype(f32)
        mine[k.slot, half2:] = k.sub(0, 1) + got[k.recv, 0, half2:].astype(f32)

    def shard2(c):
        k = Chunk(c)
        k.received(3)
        got = recv_bufs[3]
        low = mine[k.slot, :half2] + got[k.recv, 0].astype(f32)
        high = mine[k.slot, half2:] + got[k.recv, 1].astype(f32)
        k.block(0, k.q * rows2, half2)[...] = low.astype(bf16)
        k.block(0, k.q * rows2 + half2, half2)[...] = high.astype(bf16)
        k.send(4)

    def gather2(c):
        k = Chunk(c)
        k.received(4)
        k.send(5)

    def gathered2(c):
        Chunk(c).received(5)

    def gather1(c):
        Chunk(c).send(6)

    def relay_gather1(c):
        k = Chunk(c)
        k.received(6)
        k.send(7)

    def gathered1(c):
        Chunk(c).received(7)

    sends = [0, 2, 4, 6, 8, 10, 12, 15]
    steps = list(zip(sends, (multiply, relay1, shard1, relay2, shard2, gather2)))
    steps += [(12, gathered2), (sends[6], gather1), (sends[7], relay_gather1), (18, gathered1)]
    for stage, lag in enumerate(sends):
        steps.append((lag + 3, functools.partial(lambda stage, c: Chunk(c).sent(stage), stage)))

    barrier = pltpu.get_barrier_semaphore()
    here = Chunk(0)
    for pair in list(zip(a_copies(0), g_copies(0)))[:2]:
        start(pair)
    for to in (1, -1):
        for device in (here.first(to), here.second(to)):
            pl.semaphore_signal(barrier, inc=1, device_id={"dp": device}, device_id_type=pl.DeviceIdType.MESH)
    pl.semaphore_wait(barrier, 4)

    def turn(t, carry):
        for lag, do in steps:
            @pl.when((t >= lag) & (t < lag + chunks))
            def _(lag=lag, do=do):
                do(t - lag)
        return carry

    lax.fori_loop(0, chunks + max(lag for lag, _ in steps), turn, 0)


def write(sums, out, sem):
    matrices, blocks = sums.shape[:2]
    copies = [
        pltpu.make_async_copy(sums.at[n, i], out.at[n, :, i * LANES : (i + 1) * LANES], sem.at[n, i])
        for n in range(matrices)
        for i in range(blocks)
    ]
    for copy in copies:
        copy.start()
    for copy in copies:
        copy.wait()


def solution(mesh):
    side = math.isqrt(mesh.shape["dp"])

    def body(a, g):
        matrices, tokens, rows = a.shape[1:]
        columns = g.shape[3]
        width = side * LANES
        sizes = (rows, rows // 2, rows // side, rows // side // 2)
        messages = [
            pltpu.VMEM((slots, 2, size, LANES), jnp.bfloat16) for slots in (SEND_SLOTS, RECV_SLOTS) for size in sizes
        ]
        sums = pl.pallas_call(
            functools.partial(kernel, side),
            name="gradient_sums",
            out_shape=pltpu.VMEM((matrices, columns // LANES, rows, LANES), jnp.bfloat16),
            in_specs=[pl.BlockSpec(memory_space=pl.ANY)] * 2,
            out_specs=pl.BlockSpec(memory_space=pltpu.VMEM),
            scratch_shapes=[
                pltpu.VMEM((2, tokens, rows), jnp.bfloat16),
                pltpu.VMEM((G_SLOTS, tokens, width), jnp.bfloat16),
                pltpu.VMEM((rows, width), jnp.float32),
                pltpu.VMEM((SEND_SLOTS, 2, rows // 2, LANES), jnp.float32),
                pltpu.VMEM((RECV_SLOTS, rows, LANES), jnp.float32),
                pltpu.VMEM((SEND_SLOTS, rows // side, LANES), jnp.float32),
                *messages,
                pltpu.SemaphoreType.DMA((2, PIECES)),
                pltpu.SemaphoreType.DMA((G_SLOTS, PIECES)),
                pltpu.SemaphoreType.DMA((8, 2, RECV_SLOTS)),
                pltpu.SemaphoreType.DMA((8, 2, RECV_SLOTS)),
            ],
            compiler_params=pltpu.CompilerParams(
                collective_id=0, has_side_effects=True, vmem_limit_bytes=50 << 20
            ),
        )(a, g)
        return pl.pallas_call(
            write,
            name="write_sums",
            out_shape=jax.ShapeDtypeStruct((matrices, rows, columns), sums.dtype),
            in_specs=[pl.BlockSpec(memory_space=pltpu.VMEM)],
            out_specs=pl.BlockSpec(memory_space=pl.ANY),
            scratch_shapes=[pltpu.SemaphoreType.DMA((matrices, columns // LANES))],
            compiler_params=pltpu.CompilerParams(vmem_limit_bytes=1 << 20),
        )(sums)

    spec = P(("rep", "dp"), None, None, None)
    return jax.shard_map(body, mesh=mesh, in_specs=(spec, spec), out_specs=P("rep", None, None), check_vma=False)
```

```python
import functools
import math

import jax
import jax.numpy as jnp
from jax import lax
from jax.experimental import pallas as pl
from jax.experimental.pallas import tpu as pltpu
from jax.sharding import PartitionSpec as P

LANES = 128
SEND_SLOTS = 4
RECV_SLOTS = 8
PIECES = (0, 2, 6, 11, 16)
WRITES = 4
G_SLOTS = 3


def kernel(side, a_hbm, g_hbm, out, a_buf, g_buf, total, acc, part, mine, *rest):
    send_bufs, recv_bufs = rest[:4], rest[4:8]
    a_sem, g_sem, send_sem, recv_sem = rest[8:]
    matrices, tokens, rows = a_hbm.shape[1:]
    width = side * LANES
    per_matrix = g_hbm.shape[3] // width
    chunks = matrices * per_matrix
    half1, rows2 = rows // 2, rows // side
    half2 = rows2 // 2
    me, swap = lax.axis_index("dp"), lax.axis_index("rep") % 2
    x, y = me // side, me % side
    barrier = pltpu.get_barrier_semaphore()
    bf16, f32 = jnp.bfloat16, jnp.float32

    class Chunk:
        def __init__(self, c):
            odd = (c + swap) % 2
            self.c, self.slot, self.recv = c, c % SEND_SLOTS, c % RECV_SLOTS
            self.matrix = c // per_matrix
            self.column = (c % per_matrix) * width
            self.p = x * (1 - odd) + y * odd
            self.q = y * (1 - odd) + x * odd
            self.stride1 = side * (1 - odd) + odd
            self.stride2 = side * odd + 1 - odd

        def first(self, d):
            return (self.p + d + side) % side * self.stride1 + self.q * self.stride2

        def second(self, d):
            return self.p * self.stride1 + (self.q + d + side) % side * self.stride2

        def lanes(self, d):
            return pl.ds(pl.multiple_of((self.p + d + side) % side * LANES, LANES), LANES)

        def sub(self, d, half):
            s = (self.q + d + side) % side
            return part[self.recv, pl.ds(pl.multiple_of(s * rows2 + half * half2, half2), half2), :]

        def block(self, d1, start, size):
            s = (self.p + d1 + side) % side
            lanes = pl.ds(pl.multiple_of(self.column + s * LANES, LANES), LANES)
            return out.at[self.matrix, pl.ds(pl.multiple_of(start, 16), size), lanes]

        def copy(self, stage, way):
            to = 1 - 2 * way
            if stage < 4:
                src, dst = send_bufs[stage].at[self.slot, way], recv_bufs[stage].at[self.recv, way]
                device = self.first(to) if stage < 2 else self.second(to)
            elif stage == 4:
                src = dst = self.block(0, self.q * rows2, rows2)
                device = self.second(to)
            elif stage == 5:
                src = dst = self.block(0, (self.q - to + side) % side * rows2 + way * half2, half2)
                device = self.second(to)
            elif stage == 6:
                src = dst = self.block(0, 0, rows)
                device = self.first(to)
            else:
                src = dst = self.block(-to, way * half1, half1)
                device = self.first(to)
            return pltpu.make_async_remote_copy(
                src_ref=src,
                dst_ref=dst,
                send_sem=send_sem.at[stage, way, self.recv],
                recv_sem=recv_sem.at[stage, way, self.recv],
                device_id={"dp": device},
                device_id_type=pl.DeviceIdType.MESH,
            )

        def send(self, stage):
            for way in range(2):
                self.copy(stage, way).start()

        def received(self, stage):
            for way in range(2):
                self.copy(stage, way).wait_recv()

        def sent(self, stage):
            for way in range(2):
                self.copy(stage, way).wait_send()

    pieces = [slice(i * tokens // 16, j * tokens // 16) for i, j in zip(PIECES, PIECES[1:])]

    def a_copies(n):
        for i, piece in enumerate(pieces):
            yield pltpu.make_async_copy(a_hbm.at[0, n, piece, :], a_buf.at[n % 2, piece, :], a_sem.at[n % 2, i])

    def g_copies(c):
        lanes = pl.ds(pl.multiple_of(c % per_matrix * width, width), width)
        for i, piece in enumerate(pieces):
            yield pltpu.make_async_copy(
                g_hbm.at[0, c // per_matrix, piece, lanes], g_buf.at[c % G_SLOTS, piece, :], g_sem.at[c % G_SLOTS, i]
            )

    def product(k, tokens):
        g = g_buf.at[k.c % G_SLOTS]
        columns = jnp.concatenate([g[tokens, k.lanes(d)] for d in (1, 2, -1, 0)], axis=1)
        return lax.dot_general(
            a_buf[k.matrix % 2, tokens, :], columns, (((0,), (0,)), ((), ())), preferred_element_type=f32
        )

    def store(k, product):
        right, far, left, own = (product[:, i * LANES : (i + 1) * LANES] for i in range(4))
        buf = send_bufs[0]
        buf[k.slot, 0, :half1] = far[:half1].astype(bf16)
        buf[k.slot, 0, half1:] = right[half1:].astype(bf16)
        buf[k.slot, 1, :half1] = left[:half1].astype(bf16)
        buf[k.slot, 1, half1:] = far[half1:].astype(bf16)
        acc[k.slot, 0] = right[:half1]
        acc[k.slot, 1] = left[half1:]
        part[k.recv] = own

    def start(copies):
        for copy in copies:
            copy.start()

    def wait(copies):
        for copy in copies:
            copy.wait()

    def multiply(c):
        k = Chunk(c)

        @pl.when(c == 0)
        def _():
            copies = list(zip(a_copies(0), g_copies(0)))
            for i, piece in enumerate(pieces):
                wait(copies[i])
                if i + 2 < len(pieces):
                    start(copies[i + 2])
                elif i + 2 == len(pieces):
                    start(g_copies(1))
                term = product(k, piece)
                if i == 0:
                    total[...] = term
                elif i + 1 < len(pieces):
                    total[...] += term
                else:
                    store(k, total[...] + term)
            pl.semaphore_wait(barrier, 4)

        @pl.when(c > 0)
        def _():
            @pl.when(c % per_matrix == 0)
            def _():
                wait(a_copies(k.matrix))

            wait(g_copies(c))
            store(k, product(k, slice(None)))

        @pl.when((c % per_matrix == 0) & (k.matrix + 1 < matrices))
        def _():
            start(a_copies(k.matrix + 1))

        @pl.when(c + 2 < chunks)
        def _():
            start(g_copies(c + 2))

        k.send(0)

    def relay1(c):
        k = Chunk(c)
        k.received(0)
        got, buf = recv_bufs[0], send_bufs[1]
        buf[k.slot, 0] = (acc[k.slot, 0] + got[k.recv, 0, :half1].astype(f32)).astype(bf16)
        buf[k.slot, 1] = (acc[k.slot, 1] + got[k.recv, 1, half1:].astype(f32)).astype(bf16)
        k.send(1)
        part[k.recv, :half1] += got[k.recv, 1, :half1].astype(f32)
        part[k.recv, half1:] += got[k.recv, 0, half1:].astype(f32)

    def shard1(c):
        k = Chunk(c)
        k.received(1)
        got = recv_bufs[1]
        part[k.recv, :half1] += got[k.recv, 0].astype(f32)
        part[k.recv, half1:] += got[k.recv, 1].astype(f32)
        buf = send_bufs[2]
        buf[k.slot, 0, :half2] = k.sub(2, 0).astype(bf16)
        buf[k.slot, 0, half2:] = k.sub(1, 1).astype(bf16)
        buf[k.slot, 1, :half2] = k.sub(-1, 0).astype(bf16)
        buf[k.slot, 1, half2:] = k.sub(2, 1).astype(bf16)
        k.send(2)

    def relay2(c):
        k = Chunk(c)
        k.received(2)
        got, buf = recv_bufs[2], send_bufs[3]
        buf[k.slot, 0] = (k.sub(1, 0) + got[k.recv, 0, :half2].astype(f32)).astype(bf16)
        buf[k.slot, 1] = (k.sub(-1, 1) + got[k.recv, 1, half2:].astype(f32)).astype(bf16)
        k.send(3)
        mine[k.slot, :half2] = k.sub(0, 0) + got[k.recv, 1, :half2].astype(f32)
        mine[k.slot, half2:] = k.sub(0, 1) + got[k.recv, 0, half2:].astype(f32)

    def shard2(c):
        k = Chunk(c)
        k.received(3)
        got = recv_bufs[3]
        low = mine[k.slot, :half2] + got[k.recv, 0].astype(f32)
        high = mine[k.slot, half2:] + got[k.recv, 1].astype(f32)
        k.block(0, k.q * rows2, half2)[...] = low.astype(bf16)
        k.block(0, k.q * rows2 + half2, half2)[...] = high.astype(bf16)
        k.send(4)

    def gather2(c):
        k = Chunk(c)
        k.received(4)
        k.send(5)

    def gathered2(c):
        Chunk(c).received(5)

    def gather1(c):
        Chunk(c).send(6)

    def relay_gather1(c):
        k = Chunk(c)
        k.received(6)
        k.send(7)

    def gathered1(c):
        Chunk(c).received(7)

    sends = [0, 2, 4, 6, 8, 10, 12, 15]
    steps = list(zip(sends, (multiply, relay1, shard1, relay2, shard2, gather2)))
    steps += [(12, gathered2), (sends[6], gather1), (sends[7], relay_gather1), (18, gathered1)]
    for stage, lag in enumerate(sends):
        steps.append((lag + 3, functools.partial(lambda stage, c: Chunk(c).sent(stage), stage)))

    here = Chunk(0)
    for pair in list(zip(a_copies(0), g_copies(0)))[:2]:
        start(pair)
    for to in (1, -1):
        for device in (here.first(to), here.second(to)):
            pl.semaphore_signal(barrier, inc=1, device_id={"dp": device}, device_id_type=pl.DeviceIdType.MESH)

    def turn(t, carry):
        for lag, do in steps:
            @pl.when((t >= lag) & (t < lag + chunks))
            def _(lag=lag, do=do):
                do(t - lag)
        return carry

    lax.fori_loop(0, chunks + max(lag for lag, _ in steps), turn, 0)


def write(sums, out, sem):
    matrices, rows = sums.shape[:2]
    size = rows // WRITES
    copies = [
        pltpu.make_async_copy(
            sums.at[n, i * size : (i + 1) * size], out.at[n, i * size : (i + 1) * size], sem.at[n, i]
        )
        for n in range(matrices)
        for i in range(WRITES)
    ]
    for copy in copies:
        copy.start()
    for copy in copies:
        copy.wait()


def solution(mesh):
    side = math.isqrt(mesh.shape["dp"])

    def body(a, g):
        matrices, tokens, rows = a.shape[1:]
        columns = g.shape[3]
        width = side * LANES
        sizes = (rows, rows // 2, rows // side, rows // side // 2)
        messages = [
            pltpu.VMEM((slots, 2, size, LANES), jnp.bfloat16) for slots in (SEND_SLOTS, RECV_SLOTS) for size in sizes
        ]
        sums = pl.pallas_call(
            functools.partial(kernel, side),
            name="gradient_sums",
            out_shape=pltpu.VMEM((matrices, rows, columns), jnp.bfloat16),
            in_specs=[pl.BlockSpec(memory_space=pl.ANY)] * 2,
            out_specs=pl.BlockSpec(memory_space=pltpu.VMEM),
            scratch_shapes=[
                pltpu.VMEM((2, tokens, rows), jnp.bfloat16),
                pltpu.VMEM((G_SLOTS, tokens, width), jnp.bfloat16),
                pltpu.VMEM((rows, width), jnp.float32),
                pltpu.VMEM((SEND_SLOTS, 2, rows // 2, LANES), jnp.float32),
                pltpu.VMEM((RECV_SLOTS, rows, LANES), jnp.float32),
                pltpu.VMEM((SEND_SLOTS, rows // side, LANES), jnp.float32),
                *messages,
                pltpu.SemaphoreType.DMA((2, len(PIECES) - 1)),
                pltpu.SemaphoreType.DMA((G_SLOTS, len(PIECES) - 1)),
                pltpu.SemaphoreType.DMA((8, 2, RECV_SLOTS)),
                pltpu.SemaphoreType.DMA((8, 2, RECV_SLOTS)),
            ],
            compiler_params=pltpu.CompilerParams(
                collective_id=0, has_side_effects=True, vmem_limit_bytes=50 << 20
            ),
        )(a, g)
        return pl.pallas_call(
            write,
            name="write_sums",
            out_shape=jax.ShapeDtypeStruct(sums.shape, sums.dtype),
            in_specs=[pl.BlockSpec(memory_space=pltpu.VMEM)],
            out_specs=pl.BlockSpec(memory_space=pl.ANY),
            scratch_shapes=[pltpu.SemaphoreType.DMA((matrices, WRITES))],
            compiler_params=pltpu.CompilerParams(vmem_limit_bytes=1 << 20),
        )(sums)

    spec = P(("rep", "dp"), None, None, None)
    return jax.shard_map(body, mesh=mesh, in_specs=(spec, spec), out_specs=P("rep", None, None), check_vma=False)
```

```python
import functools
import math

import jax
import jax.numpy as jnp
from jax import lax
from jax.experimental import pallas as pl
from jax.experimental.pallas import tpu as pltpu
from jax.sharding import PartitionSpec as P

LANES = 128
SEND_SLOTS = 4
RECV_SLOTS = 8
SEM_SLOTS = 12
PIECES = (0, 2, 6, 11, 16)
WRITES = 4
G_SLOTS = 3


def kernel(side, a_hbm, g_hbm, out, a_buf, g_buf, total, acc, part, mine, *rest):
    send_bufs, recv_bufs = rest[:4], rest[4:8]
    a_sem, g_sem, send_sem, recv_sem = rest[8:]
    matrices, tokens, rows = a_hbm.shape[1:]
    width = side * LANES
    per_matrix = g_hbm.shape[3] // width
    chunks = matrices * per_matrix
    half1, rows2 = rows // 2, rows // side
    half2 = rows2 // 2
    me, swap = lax.axis_index("dp"), lax.axis_index("rep") % 2
    x, y = me // side, me % side
    barrier = pltpu.get_barrier_semaphore()
    bf16, f32 = jnp.bfloat16, jnp.float32

    class Chunk:
        def __init__(self, c):
            odd = (c + swap) % 2
            self.c, self.slot, self.recv, self.sem = c, c % SEND_SLOTS, c % RECV_SLOTS, c % SEM_SLOTS
            self.matrix = c // per_matrix
            self.column = (c % per_matrix) * width
            self.p = x * (1 - odd) + y * odd
            self.q = y * (1 - odd) + x * odd
            self.stride1 = side * (1 - odd) + odd
            self.stride2 = side * odd + 1 - odd

        def first(self, d):
            return (self.p + d + side) % side * self.stride1 + self.q * self.stride2

        def second(self, d):
            return self.p * self.stride1 + (self.q + d + side) % side * self.stride2

        def lanes(self, d):
            return pl.ds(pl.multiple_of((self.p + d + side) % side * LANES, LANES), LANES)

        def sub(self, d, half):
            s = (self.q + d + side) % side
            return part[self.recv, pl.ds(pl.multiple_of(s * rows2 + half * half2, half2), half2), :]

        def block(self, d1, start, size):
            s = (self.p + d1 + side) % side
            lanes = pl.ds(pl.multiple_of(self.column + s * LANES, LANES), LANES)
            return out.at[self.matrix, pl.ds(pl.multiple_of(start, 16), size), lanes]

        def copy(self, stage, way):
            to = 1 - 2 * way
            if stage < 4:
                src, dst = send_bufs[stage].at[self.slot, way], recv_bufs[stage].at[self.recv, way]
                device = self.first(to) if stage < 2 else self.second(to)
            elif stage == 4:
                src = dst = self.block(0, self.q * rows2, rows2)
                device = self.second(to)
            elif stage == 5:
                src = dst = self.block(0, (self.q - to + side) % side * rows2 + way * half2, half2)
                device = self.second(to)
            elif stage == 6:
                src = dst = self.block(0, 0, rows)
                device = self.first(to)
            else:
                src = dst = self.block(-to, way * half1, half1)
                device = self.first(to)
            return pltpu.make_async_remote_copy(
                src_ref=src,
                dst_ref=dst,
                send_sem=send_sem.at[stage, way, self.sem],
                recv_sem=recv_sem.at[stage, way, self.sem],
                device_id={"dp": device},
                device_id_type=pl.DeviceIdType.MESH,
            )

        def send(self, stage):
            for way in range(2):
                self.copy(stage, way).start()

        def received(self, stage):
            for way in range(2):
                self.copy(stage, way).wait_recv()

        def sent(self, stage):
            for way in range(2):
                self.copy(stage, way).wait_send()

    pieces = [slice(i * tokens // 16, j * tokens // 16) for i, j in zip(PIECES, PIECES[1:])]

    def a_copies(n):
        for i, piece in enumerate(pieces):
            yield pltpu.make_async_copy(a_hbm.at[0, n, piece, :], a_buf.at[n % 2, piece, :], a_sem.at[n % 2, i])

    def g_copies(c):
        lanes = pl.ds(pl.multiple_of(c % per_matrix * width, width), width)
        for i, piece in enumerate(pieces):
            yield pltpu.make_async_copy(
                g_hbm.at[0, c // per_matrix, piece, lanes], g_buf.at[c % G_SLOTS, piece, :], g_sem.at[c % G_SLOTS, i]
            )

    def product(k, tokens):
        g = g_buf.at[k.c % G_SLOTS]
        columns = jnp.concatenate([g[tokens, k.lanes(d)] for d in (1, 2, -1, 0)], axis=1)
        return lax.dot_general(
            a_buf[k.matrix % 2, tokens, :], columns, (((0,), (0,)), ((), ())), preferred_element_type=f32
        )

    def store(k, product):
        right, far, left, own = (product[:, i * LANES : (i + 1) * LANES] for i in range(4))
        buf = send_bufs[0]
        buf[k.slot, 0, :half1] = far[:half1].astype(bf16)
        buf[k.slot, 0, half1:] = right[half1:].astype(bf16)
        buf[k.slot, 1, :half1] = left[:half1].astype(bf16)
        buf[k.slot, 1, half1:] = far[half1:].astype(bf16)
        acc[k.slot, 0] = right[:half1]
        acc[k.slot, 1] = left[half1:]
        part[k.recv] = own

    def start(copies):
        for copy in copies:
            copy.start()

    def wait(copies):
        for copy in copies:
            copy.wait()

    def multiply(c):
        k = Chunk(c)

        @pl.when(c == 0)
        def _():
            copies = list(zip(a_copies(0), g_copies(0)))
            for i, piece in enumerate(pieces):
                wait(copies[i])
                if i + 2 < len(pieces):
                    start(copies[i + 2])
                elif i + 2 == len(pieces):
                    start(g_copies(1))
                term = product(k, piece)
                if i == 0:
                    total[...] = term
                elif i + 1 < len(pieces):
                    total[...] += term
                else:
                    store(k, total[...] + term)
            pl.semaphore_wait(barrier, 4)

        @pl.when(c > 0)
        def _():
            @pl.when(c % per_matrix == 0)
            def _():
                wait(a_copies(k.matrix))

            wait(g_copies(c))
            store(k, product(k, slice(None)))

        @pl.when((c % per_matrix == 0) & (k.matrix + 1 < matrices))
        def _():
            start(a_copies(k.matrix + 1))

        @pl.when(c + 2 < chunks)
        def _():
            start(g_copies(c + 2))

        k.send(0)

    def relay1(c):
        k = Chunk(c)
        k.received(0)
        got, buf = recv_bufs[0], send_bufs[1]
        buf[k.slot, 0] = (acc[k.slot, 0] + got[k.recv, 0, :half1].astype(f32)).astype(bf16)
        buf[k.slot, 1] = (acc[k.slot, 1] + got[k.recv, 1, half1:].astype(f32)).astype(bf16)
        k.send(1)
        part[k.recv, :half1] += got[k.recv, 1, :half1].astype(f32)
        part[k.recv, half1:] += got[k.recv, 0, half1:].astype(f32)

    def shard1(c):
        k = Chunk(c)
        k.received(1)
        got = recv_bufs[1]
        part[k.recv, :half1] += got[k.recv, 0].astype(f32)
        part[k.recv, half1:] += got[k.recv, 1].astype(f32)
        buf = send_bufs[2]
        buf[k.slot, 0, :half2] = k.sub(2, 0).astype(bf16)
        buf[k.slot, 0, half2:] = k.sub(1, 1).astype(bf16)
        buf[k.slot, 1, :half2] = k.sub(-1, 0).astype(bf16)
        buf[k.slot, 1, half2:] = k.sub(2, 1).astype(bf16)
        k.send(2)

    def relay2(c):
        k = Chunk(c)
        k.received(2)
        got, buf = recv_bufs[2], send_bufs[3]
        buf[k.slot, 0] = (k.sub(1, 0) + got[k.recv, 0, :half2].astype(f32)).astype(bf16)
        buf[k.slot, 1] = (k.sub(-1, 1) + got[k.recv, 1, half2:].astype(f32)).astype(bf16)
        k.send(3)
        mine[k.slot, :half2] = k.sub(0, 0) + got[k.recv, 1, :half2].astype(f32)
        mine[k.slot, half2:] = k.sub(0, 1) + got[k.recv, 0, half2:].astype(f32)

    def shard2(c):
        k = Chunk(c)
        k.received(3)
        got = recv_bufs[3]
        low = mine[k.slot, :half2] + got[k.recv, 0].astype(f32)
        high = mine[k.slot, half2:] + got[k.recv, 1].astype(f32)
        k.block(0, k.q * rows2, half2)[...] = low.astype(bf16)
        k.block(0, k.q * rows2 + half2, half2)[...] = high.astype(bf16)
        k.send(4)

    def gather2(c):
        k = Chunk(c)
        k.received(4)
        k.send(5)

    def gathered2(c):
        Chunk(c).received(5)

    def gather1(c):
        Chunk(c).send(6)

    def relay_gather1(c):
        k = Chunk(c)
        k.received(6)
        k.send(7)

    def gathered1(c):
        Chunk(c).received(7)

    sends = [0, 2, 4, 6, 8, 10, 12, 17]
    steps = list(zip(sends, (multiply, relay1, shard1, relay2, shard2, gather2)))
    steps += [(12, gathered2), (sends[6], gather1), (sends[7], relay_gather1), (22, gathered1)]
    for stage, lag in enumerate(sends):
        steps.append((lag + 3, functools.partial(lambda stage, c: Chunk(c).sent(stage), stage)))

    here = Chunk(0)
    for pair in list(zip(a_copies(0), g_copies(0)))[:2]:
        start(pair)
    for to in (1, -1):
        for device in (here.first(to), here.second(to)):
            pl.semaphore_signal(barrier, inc=1, device_id={"dp": device}, device_id_type=pl.DeviceIdType.MESH)

    def turn(t, carry):
        for lag, do in steps:
            @pl.when((t >= lag) & (t < lag + chunks))
            def _(lag=lag, do=do):
                do(t - lag)
        return carry

    lax.fori_loop(0, chunks + max(lag for lag, _ in steps), turn, 0)


def write(sums, out, sem):
    matrices, rows = sums.shape[:2]
    size = rows // WRITES
    copies = [
        pltpu.make_async_copy(
            sums.at[n, i * size : (i + 1) * size], out.at[n, i * size : (i + 1) * size], sem.at[n, i]
        )
        for n in range(matrices)
        for i in range(WRITES)
    ]
    for copy in copies:
        copy.start()
    for copy in copies:
        copy.wait()


def solution(mesh):
    side = math.isqrt(mesh.shape["dp"])

    def body(a, g):
        matrices, tokens, rows = a.shape[1:]
        columns = g.shape[3]
        width = side * LANES
        sizes = (rows, rows // 2, rows // side, rows // side // 2)
        messages = [
            pltpu.VMEM((slots, 2, size, LANES), jnp.bfloat16) for slots in (SEND_SLOTS, RECV_SLOTS) for size in sizes
        ]
        sums = pl.pallas_call(
            functools.partial(kernel, side),
            name="gradient_sums",
            out_shape=pltpu.VMEM((matrices, rows, columns), jnp.bfloat16),
            in_specs=[pl.BlockSpec(memory_space=pl.ANY)] * 2,
            out_specs=pl.BlockSpec(memory_space=pltpu.VMEM),
            scratch_shapes=[
                pltpu.VMEM((2, tokens, rows), jnp.bfloat16),
                pltpu.VMEM((G_SLOTS, tokens, width), jnp.bfloat16),
                pltpu.VMEM((rows, width), jnp.float32),
                pltpu.VMEM((SEND_SLOTS, 2, rows // 2, LANES), jnp.float32),
                pltpu.VMEM((RECV_SLOTS, rows, LANES), jnp.float32),
                pltpu.VMEM((SEND_SLOTS, rows // side, LANES), jnp.float32),
                *messages,
                pltpu.SemaphoreType.DMA((2, len(PIECES) - 1)),
                pltpu.SemaphoreType.DMA((G_SLOTS, len(PIECES) - 1)),
                pltpu.SemaphoreType.DMA((8, 2, SEM_SLOTS)),
                pltpu.SemaphoreType.DMA((8, 2, SEM_SLOTS)),
            ],
            compiler_params=pltpu.CompilerParams(
                collective_id=0, has_side_effects=True, vmem_limit_bytes=50 << 20
            ),
        )(a, g)
        return pl.pallas_call(
            write,
            name="write_sums",
            out_shape=jax.ShapeDtypeStruct(sums.shape, sums.dtype),
            in_specs=[pl.BlockSpec(memory_space=pltpu.VMEM)],
            out_specs=pl.BlockSpec(memory_space=pl.ANY),
            scratch_shapes=[pltpu.SemaphoreType.DMA((matrices, WRITES))],
            compiler_params=pltpu.CompilerParams(vmem_limit_bytes=1 << 20),
        )(sums)

    spec = P(("rep", "dp"), None, None, None)
    return jax.shard_map(body, mesh=mesh, in_specs=(spec, spec), out_specs=P("rep", None, None), check_vma=False)
```

```python
import functools
import math

import jax
import jax.numpy as jnp
from jax import lax
from jax.experimental import pallas as pl
from jax.experimental.pallas import tpu as pltpu
from jax.sharding import PartitionSpec as P

LANES = 128
SEND_SLOTS = 4
RECV_SLOTS = 8
PIECES = (0, 2, 6, 11, 16)
WRITES = 8
G_SLOTS = 3


def kernel(side, a_hbm, g_hbm, out, a_buf, g_buf, total, acc, part, mine, *rest):
    send_bufs, recv_bufs = rest[:4], rest[4:8]
    a_sem, g_sem, send_sem, recv_sem = rest[8:]
    matrices, tokens, rows = a_hbm.shape[1:]
    width = side * LANES
    per_matrix = g_hbm.shape[3] // width
    chunks = matrices * per_matrix
    half1, rows2 = rows // 2, rows // side
    half2 = rows2 // 2
    me, swap = lax.axis_index("dp"), lax.axis_index("rep") % 2
    x, y = me // side, me % side
    barrier = pltpu.get_barrier_semaphore()
    bf16, f32 = jnp.bfloat16, jnp.float32

    class Chunk:
        def __init__(self, c):
            odd = (c + swap) % 2
            self.c, self.slot, self.recv = c, c % SEND_SLOTS, c % RECV_SLOTS
            self.matrix = c // per_matrix
            self.column = (c % per_matrix) * width
            self.p = x * (1 - odd) + y * odd
            self.q = y * (1 - odd) + x * odd
            self.stride1 = side * (1 - odd) + odd
            self.stride2 = side * odd + 1 - odd

        def first(self, d):
            return (self.p + d + side) % side * self.stride1 + self.q * self.stride2

        def second(self, d):
            return self.p * self.stride1 + (self.q + d + side) % side * self.stride2

        def lanes(self, d):
            return pl.ds(pl.multiple_of((self.p + d + side) % side * LANES, LANES), LANES)

        def sub(self, d, half):
            s = (self.q + d + side) % side
            return part[self.recv, pl.ds(pl.multiple_of(s * rows2 + half * half2, half2), half2), :]

        def block(self, d1, start, size):
            s = (self.p + d1 + side) % side
            lanes = pl.ds(pl.multiple_of(self.column + s * LANES, LANES), LANES)
            return out.at[self.matrix, pl.ds(pl.multiple_of(start, 16), size), lanes]

        def copy(self, stage, way):
            to = 1 - 2 * way
            if stage < 4:
                src, dst = send_bufs[stage].at[self.slot, way], recv_bufs[stage].at[self.recv, way]
                device = self.first(to) if stage < 2 else self.second(to)
            elif stage == 4:
                src = dst = self.block(0, self.q * rows2, rows2)
                device = self.second(to)
            elif stage == 5:
                src = dst = self.block(0, (self.q - to + side) % side * rows2 + way * half2, half2)
                device = self.second(to)
            elif stage == 6:
                src = dst = self.block(0, 0, rows)
                device = self.first(to)
            else:
                src = dst = self.block(-to, way * half1, half1)
                device = self.first(to)
            return pltpu.make_async_remote_copy(
                src_ref=src,
                dst_ref=dst,
                send_sem=send_sem.at[stage, way, self.recv],
                recv_sem=recv_sem.at[stage, way, self.recv],
                device_id={"dp": device},
                device_id_type=pl.DeviceIdType.MESH,
            )

        def send(self, stage):
            for way in range(2):
                self.copy(stage, way).start()

        def received(self, stage):
            for way in range(2):
                self.copy(stage, way).wait_recv()

        def sent(self, stage):
            for way in range(2):
                self.copy(stage, way).wait_send()

    pieces = [slice(i * tokens // 16, j * tokens // 16) for i, j in zip(PIECES, PIECES[1:])]

    def a_copies(n):
        for i, piece in enumerate(pieces):
            yield pltpu.make_async_copy(a_hbm.at[0, n, piece, :], a_buf.at[n % 2, piece, :], a_sem.at[n % 2, i])

    def g_copies(c):
        lanes = pl.ds(pl.multiple_of(c % per_matrix * width, width), width)
        for i, piece in enumerate(pieces):
            yield pltpu.make_async_copy(
                g_hbm.at[0, c // per_matrix, piece, lanes], g_buf.at[c % G_SLOTS, piece, :], g_sem.at[c % G_SLOTS, i]
            )

    def product(k, tokens):
        g = g_buf.at[k.c % G_SLOTS]
        columns = jnp.concatenate([g[tokens, k.lanes(d)] for d in (1, 2, -1, 0)], axis=1)
        return lax.dot_general(
            a_buf[k.matrix % 2, tokens, :], columns, (((0,), (0,)), ((), ())), preferred_element_type=f32
        )

    def store(k, product):
        right, far, left, own = (product[:, i * LANES : (i + 1) * LANES] for i in range(4))
        buf = send_bufs[0]
        buf[k.slot, 0, :half1] = far[:half1].astype(bf16)
        buf[k.slot, 0, half1:] = right[half1:].astype(bf16)
        buf[k.slot, 1, :half1] = left[:half1].astype(bf16)
        buf[k.slot, 1, half1:] = far[half1:].astype(bf16)
        acc[k.slot, 0] = right[:half1]
        acc[k.slot, 1] = left[half1:]
        part[k.recv] = own

    def start(copies):
        for copy in copies:
            copy.start()

    def wait(copies):
        for copy in copies:
            copy.wait()

    def multiply(c):
        k = Chunk(c)

        @pl.when(c == 0)
        def _():
            copies = list(zip(a_copies(0), g_copies(0)))
            for i, piece in enumerate(pieces):
                wait(copies[i])
                if i + 2 < len(pieces):
                    start(copies[i + 2])
                elif i + 2 == len(pieces):
                    start(g_copies(1))
                term = product(k, piece)
                if i == 0:
                    total[...] = term
                elif i + 1 < len(pieces):
                    total[...] += term
                else:
                    store(k, total[...] + term)
            pl.semaphore_wait(barrier, 4)

        @pl.when(c > 0)
        def _():
            @pl.when(c % per_matrix == 0)
            def _():
                wait(a_copies(k.matrix))

            wait(g_copies(c))
            store(k, product(k, slice(None)))

        @pl.when((c % per_matrix == 0) & (k.matrix + 1 < matrices))
        def _():
            start(a_copies(k.matrix + 1))

        @pl.when(c + 2 < chunks)
        def _():
            start(g_copies(c + 2))

        k.send(0)

    def relay1(c):
        k = Chunk(c)
        k.received(0)
        got, buf = recv_bufs[0], send_bufs[1]
        buf[k.slot, 0] = (acc[k.slot, 0] + got[k.recv, 0, :half1].astype(f32)).astype(bf16)
        buf[k.slot, 1] = (acc[k.slot, 1] + got[k.recv, 1, half1:].astype(f32)).astype(bf16)
        k.send(1)
        part[k.recv, :half1] += got[k.recv, 1, :half1].astype(f32)
        part[k.recv, half1:] += got[k.recv, 0, half1:].astype(f32)

    def shard1(c):
        k = Chunk(c)
        k.received(1)
        got = recv_bufs[1]
        part[k.recv, :half1] += got[k.recv, 0].astype(f32)
        part[k.recv, half1:] += got[k.recv, 1].astype(f32)
        buf = send_bufs[2]
        buf[k.slot, 0, :half2] = k.sub(2, 0).astype(bf16)
        buf[k.slot, 0, half2:] = k.sub(1, 1).astype(bf16)
        buf[k.slot, 1, :half2] = k.sub(-1, 0).astype(bf16)
        buf[k.slot, 1, half2:] = k.sub(2, 1).astype(bf16)
        k.send(2)

    def relay2(c):
        k = Chunk(c)
        k.received(2)
        got, buf = recv_bufs[2], send_bufs[3]
        buf[k.slot, 0] = (k.sub(1, 0) + got[k.recv, 0, :half2].astype(f32)).astype(bf16)
        buf[k.slot, 1] = (k.sub(-1, 1) + got[k.recv, 1, half2:].astype(f32)).astype(bf16)
        k.send(3)
        mine[k.slot, :half2] = k.sub(0, 0) + got[k.recv, 1, :half2].astype(f32)
        mine[k.slot, half2:] = k.sub(0, 1) + got[k.recv, 0, half2:].astype(f32)

    def shard2(c):
        k = Chunk(c)
        k.received(3)
        got = recv_bufs[3]
        low = mine[k.slot, :half2] + got[k.recv, 0].astype(f32)
        high = mine[k.slot, half2:] + got[k.recv, 1].astype(f32)
        k.block(0, k.q * rows2, half2)[...] = low.astype(bf16)
        k.block(0, k.q * rows2 + half2, half2)[...] = high.astype(bf16)
        k.send(4)

    def gather2(c):
        k = Chunk(c)
        k.received(4)
        k.send(5)

    def gathered2(c):
        Chunk(c).received(5)

    def gather1(c):
        Chunk(c).send(6)

    def relay_gather1(c):
        k = Chunk(c)
        k.received(6)
        k.send(7)

    def gathered1(c):
        Chunk(c).received(7)

    sends = [0, 2, 4, 6, 8, 10, 12, 14]
    steps = list(zip(sends, (multiply, relay1, shard1, relay2, shard2, gather2)))
    steps += [(12, gathered2), (sends[6], gather1), (sends[7], relay_gather1), (16, gathered1)]
    for stage, lag in enumerate(sends):
        steps.append((lag + 3, functools.partial(lambda stage, c: Chunk(c).sent(stage), stage)))

    here = Chunk(0)
    for pair in list(zip(a_copies(0), g_copies(0)))[:2]:
        start(pair)
    for to in (1, -1):
        for device in (here.first(to), here.second(to)):
            pl.semaphore_signal(barrier, inc=1, device_id={"dp": device}, device_id_type=pl.DeviceIdType.MESH)

    def turn(t, carry):
        for lag, do in steps:
            @pl.when((t >= lag) & (t < lag + chunks))
            def _(lag=lag, do=do):
                do(t - lag)
        return carry

    lax.fori_loop(0, chunks + max(lag for lag, _ in steps), turn, 0)


def write(sums, out, sem):
    matrices, rows = sums.shape[:2]
    size = rows // WRITES
    copies = [
        pltpu.make_async_copy(
            sums.at[n, i * size : (i + 1) * size], out.at[n, i * size : (i + 1) * size], sem.at[n, i]
        )
        for n in range(matrices)
        for i in range(WRITES)
    ]
    for copy in copies:
        copy.start()
    for copy in copies:
        copy.wait()


def solution(mesh):
    side = math.isqrt(mesh.shape["dp"])

    def body(a, g):
        matrices, tokens, rows = a.shape[1:]
        columns = g.shape[3]
        width = side * LANES
        sizes = (rows, rows // 2, rows // side, rows // side // 2)
        messages = [
            pltpu.VMEM((slots, 2, size, LANES), jnp.bfloat16) for slots in (SEND_SLOTS, RECV_SLOTS) for size in sizes
        ]
        sums = pl.pallas_call(
            functools.partial(kernel, side),
            name="gradient_sums",
            out_shape=pltpu.VMEM((matrices, rows, columns), jnp.bfloat16),
            in_specs=[pl.BlockSpec(memory_space=pl.ANY)] * 2,
            out_specs=pl.BlockSpec(memory_space=pltpu.VMEM),
            scratch_shapes=[
                pltpu.VMEM((2, tokens, rows), jnp.bfloat16),
                pltpu.VMEM((G_SLOTS, tokens, width), jnp.bfloat16),
                pltpu.VMEM((rows, width), jnp.float32),
                pltpu.VMEM((SEND_SLOTS, 2, rows // 2, LANES), jnp.float32),
                pltpu.VMEM((RECV_SLOTS, rows, LANES), jnp.float32),
                pltpu.VMEM((SEND_SLOTS, rows // side, LANES), jnp.float32),
                *messages,
                pltpu.SemaphoreType.DMA((2, len(PIECES) - 1)),
                pltpu.SemaphoreType.DMA((G_SLOTS, len(PIECES) - 1)),
                pltpu.SemaphoreType.DMA((8, 2, RECV_SLOTS)),
                pltpu.SemaphoreType.DMA((8, 2, RECV_SLOTS)),
            ],
            compiler_params=pltpu.CompilerParams(
                collective_id=0, has_side_effects=True, vmem_limit_bytes=50 << 20
            ),
        )(a, g)
        return pl.pallas_call(
            write,
            name="write_sums",
            out_shape=jax.ShapeDtypeStruct(sums.shape, sums.dtype),
            in_specs=[pl.BlockSpec(memory_space=pltpu.VMEM)],
            out_specs=pl.BlockSpec(memory_space=pl.ANY),
            scratch_shapes=[pltpu.SemaphoreType.DMA((matrices, WRITES))],
            compiler_params=pltpu.CompilerParams(vmem_limit_bytes=1 << 20),
        )(sums)

    spec = P(("rep", "dp"), None, None, None)
    return jax.shard_map(body, mesh=mesh, in_specs=(spec, spec), out_specs=P("rep", None, None), check_vma=False)
```
